32 devices in a mesh: fsdp: 4 (over y, core), sp: 8 (over z, x).
Axes of the slice: x: 2, y: 2, z: 4, core: 2. Of those that a mesh axis runs over, the one named last changes fastest.
Arguments:
- hidden: bfloat16 [2048, 8192], P('sp', 'fsdp'), may hold values from -23 to 23
- w_query: bfloat16 [8192, 1024], P('fsdp', 'sp'), may hold values from -0.125 to 0.125
- w_keyvalue: bfloat16 [8192, 256], P('fsdp', 'sp'), may hold values from -0.125 to 0.125
- w_output: bfloat16 [1024, 8192], P('sp', 'fsdp'), may hold values from -0.75 to 0.75
- segment_ids: int32 [2048], P('sp'), may hold values from 0 to 7, never falling along the last dimension, each value on 1 to 512 neighbouring positions
Outputs:
- attended: bfloat16 [2048, 8192], P('sp', 'fsdp')
The draws below stay inside these ranges and needn't reach their ends.
Inputs may be any that keep to these rules, and one draw needn't show every extreme that they name: `segment_ids`: segment ids never fall along the sequence; every episode has between 1 and 512 tokens.
All inputs are finite; a program needn't handle non-finite values.
Results may differ from the reference program's by a relative error of at most 0.0085.
The reference program's roundings to bfloat16 on the way count: a program that leaves them out, or rounds other values in their place, can miss the bound.
Values may be sent and summed in bfloat16 or wider, within the bound.
No kernel may reach another device: no remote copies, remote signals or barrier semaphores. Data moves between devices by JAX's collectives and lax.ppermute only.
A program may use at most 128 MiB of HBM per device.

```python
import math
import jax
import jax.numpy as jnp
import numpy as np
from jax import lax

D = 8192
HD = 128
GROUP = 8
HEADS = 8
KV_HEADS = 1
SEQ = 2048


def draw_hidden(key, part):
    base_key = jax.random.fold_in(jax.random.fold_in(key, 11), 0)
    entries = jnp.clip(jax.random.normal(base_key, (SEQ, D), jnp.float32), -6.0, 6.0)
    return entries.astype(jnp.bfloat16)


def steps_of(own_key, shape, pieces, low, largest):
    def one(position, blocks):
        heights = jax.random.uniform(jax.random.fold_in(jax.random.fold_in(own_key, 6), position), (blocks,), jnp.float32, low / len(pieces), largest / len(pieces))
        return jnp.repeat(jnp.exp(heights), shape[position] // blocks).reshape((-1,) + (1,) * (len(shape) - position - 1))

    loudness = one(*pieces[0])
    for cut in pieces[1:]:
        loudness = loudness * one(*cut)
    return loudness


def profile(count, total, limit, slope):
    weights = [(1 << 20) // math.isqrt(grade ** slope) + 1 for grade in range(2, count + 1)]
    surplus, holding = total - limit - (count - 1), [1] * (count - 1)
    while surplus > 0:
        candidates = [i for i in range(count - 1) if holding[i] < limit]
        pool, remaining = sum([weights[i] for i in candidates]), surplus
        for i in candidates:
            addition = min(limit - holding[i], max(1, remaining * weights[i] // pool), surplus)
            holding[i] = holding[i] + addition
            surplus = surplus - addition
    return np.array([limit] + holding)


def ragged_sizes(own_key, number_of, total, reach, skew):
    if number_of == 2:
        one = jax.random.randint(own_key, (), max(1, total - reach), min(reach, total - 1) + 1)
        return jnp.stack([one, total - one])
    lengths = jnp.asarray(profile(number_of, total, reach, skew), jnp.int32)
    couples = (number_of - 1) // 2
    source_of, sink = lengths[1:1 + 2 * couples:2], lengths[2:2 + 2 * couples:2]
    room = jnp.minimum(source_of - 1, reach - sink)
    shifted = jax.random.randint(jax.random.fold_in(own_key, 1), (couples,), 0, 1 << 20) % (room + 1)
    lengths = lengths.at[1:1 + 2 * couples:2].set(source_of - shifted).at[2:2 + 2 * couples:2].set(sink + shifted)
    return lengths[jax.random.permutation(jax.random.fold_in(own_key, 2), number_of)]


def scatter_about(own_key, dims, spread, bound, pieces=(), held_as=jnp.bfloat16):
    values = jax.random.normal(own_key, dims, jnp.float32) * spread
    if len(pieces) > 0:
        values = steps_of(own_key, dims, pieces, -0.22, 0.18) * values
    return jnp.clip(values, min=-bound, max=bound).astype(held_as)


def setup_inputs(seed: int = 0) -> dict:
    arg_keys = jax.random.split(jax.random.key(seed), 6)
    return {
        "hidden": draw_hidden(jax.random.fold_in(arg_keys[5], 71), 0),
        "w_query": scatter_about(arg_keys[1], (D, HEADS * HD), (D // 4) ** -0.5, 0.125, ((0, 4), (1, 8))),
        "w_keyvalue": scatter_about(arg_keys[2], (D, 2 * KV_HEADS * HD), (D // 4) ** -0.5, 0.125, ((0, 4), (1, 8))),
        "w_output": scatter_about(arg_keys[3], (HEADS * HD, D), (HEADS * HD // 16) ** -0.5, 0.75, ((0, 8), (1, 4))),
        "segment_ids": jnp.searchsorted(jnp.cumsum(ragged_sizes(arg_keys[4], 8, SEQ, SEQ // 4, 0)), jnp.arange(SEQ), side="right").astype(jnp.int32),
    }


ROPE_BASE = 500000.0
NEG_FILL = -1.0e30


def rotate(values, positions, head_count, width):
    row_count = values.shape[0]
    shaped = values.reshape(row_count, head_count, width)
    half_width = width // 2
    frequency = jnp.exp(jnp.arange(half_width, dtype=jnp.float32) * (-2.0 * math.log(ROPE_BASE) / width))
    angles = positions.astype(jnp.float32)[:, None] * frequency[None, :]
    cosine = jnp.cos(angles)[:, None, :]
    sine_part = jnp.sin(angles)[:, None, :]
    lower_half = shaped[:, :, :half_width]
    upper_half = shaped[:, :, half_width:]
    turned = jnp.concatenate([lower_half * cosine - upper_half * sine_part, upper_half * cosine + lower_half * sine_part], axis=2)
    return turned.reshape(row_count, head_count * width)


def split_keys(kv_sum, positions, kv_count, width):
    row_count = kv_sum.shape[0]
    shaped = kv_sum.reshape(row_count, kv_count, 2, width)
    key_part = rotate(shaped[:, :, 0, :].reshape(row_count, kv_count * width), positions, kv_count, width)
    key_part = key_part.reshape(row_count, kv_count, 1, width)
    return jnp.concatenate([key_part, shaped[:, :, 1:2, :]], axis=2).astype(jnp.bfloat16)


def reference(hidden, w_query, w_keyvalue, w_output, segment_ids):
    seq_len = hidden.shape[0]
    positions = jnp.arange(seq_len, dtype=jnp.int32)
    query = rotate(jnp.dot(hidden, w_query, preferred_element_type=jnp.float32), positions, HEADS, HD).astype(jnp.bfloat16)
    pairs = split_keys(jnp.dot(hidden, w_keyvalue, preferred_element_type=jnp.float32), positions, KV_HEADS, HD)
    key_all = pairs[:, :, 0, :]
    value_all = pairs[:, :, 1, :]
    block_len = min(512, seq_len)
    block_count = seq_len // block_len
    score_scale = HD ** -0.5

    def one_block(item_index):
        head_id = item_index // block_count
        block_id = item_index % block_count
        first_row = (block_id * block_len).astype(jnp.int32)
        query_block = lax.dynamic_slice(query, (first_row, (head_id * HD).astype(jnp.int32)), (block_len, HD))
        group_id = (head_id // GROUP).astype(jnp.int32)
        key_block = lax.dynamic_index_in_dim(key_all, group_id, axis=1, keepdims=False)
        value_block = lax.dynamic_index_in_dim(value_all, group_id, axis=1, keepdims=False)
        scores = lax.dot_general(query_block, key_block, (((1,), (1,)), ((), ())), preferred_element_type=jnp.float32) * score_scale
        query_pos = first_row + jnp.arange(block_len, dtype=jnp.int32)
        query_seg = lax.dynamic_slice_in_dim(segment_ids, first_row, block_len)
        allowed = (positions[None, :] <= query_pos[:, None]) & (segment_ids[None, :] == query_seg[:, None])
        masked = jnp.where(allowed, scores, NEG_FILL)
        row_max = jnp.max(masked, axis=1, keepdims=True)
        weights = jnp.where(allowed, jnp.exp(masked - row_max), 0.0)
        row_total = jnp.sum(weights, axis=1, keepdims=True)
        mixed_block = jnp.dot(weights.astype(jnp.bfloat16), value_block, preferred_element_type=jnp.float32)
        return (mixed_block / row_total).astype(jnp.bfloat16)

    blocks = lax.map(one_block, jnp.arange(HEADS * block_count, dtype=jnp.int32))
    mixed = blocks.reshape(HEADS, seq_len, HD).transpose(1, 0, 2).reshape(seq_len, HEADS * HD)
    return jnp.dot(mixed, w_output, preferred_element_type=jnp.float32).astype(jnp.bfloat16)
```

```python
import math

import jax
import jax.numpy as jnp
from jax import lax
from jax.sharding import PartitionSpec as P

HD = 128
GROUP = 8


ROPE_BASE = 500000.0
NEG_FILL = -1e30


def rotate(values, positions, head_count, width):
    row_count = values.shape[0]
    shaped = values.reshape(row_count, head_count, width)
    half_width = width // 2
    frequency = jnp.exp(
        jnp.arange(half_width, dtype=jnp.float32) * (-2.0 * math.log(ROPE_BASE) / width)
    )
    angles = positions.astype(jnp.float32)[:, None] * frequency[None, :]
    cosine = jnp.cos(angles)[:, None, :]
    sine_part = jnp.sin(angles)[:, None, :]
    lower_half = shaped[:, :, :half_width]
    upper_half = shaped[:, :, half_width:]
    turned = jnp.concatenate(
        [
            lower_half * cosine - upper_half * sine_part,
            upper_half * cosine + lower_half * sine_part,
        ],
        axis=2,
    )
    return turned.reshape(row_count, head_count * width)


def split_keys(kv_sum, positions, kv_count, width):
    row_count = kv_sum.shape[0]
    shaped = kv_sum.reshape(row_count, kv_count, 2, width)
    key_part = rotate(
        shaped[:, :, 0, :].reshape(row_count, kv_count * width), positions, kv_count, width
    )
    key_part = key_part.reshape(row_count, kv_count, 1, width)
    return jnp.concatenate([key_part, shaped[:, :, 1:2, :]], axis=2).astype(jnp.bfloat16)


def merge_keys(
    state_in, query_tile, query_pos_tile, query_seg_tile, key_tile, key_pos_tile, key_seg_tile
):
    running_max, running_sum, weighted = state_in
    allowed = (key_pos_tile[None, :] <= query_pos_tile[:, None]) & (
        key_seg_tile[None, :] == query_seg_tile[:, None]
    )
    key_part = key_tile[:, :HD]
    value_part = key_tile[:, HD:]
    scores = lax.dot_general(
        query_tile, key_part, (((1,), (1,)), ((), ())), preferred_element_type=jnp.float32
    ) * HD ** (-0.5)
    masked = jnp.where(allowed, scores, NEG_FILL)
    new_max = jnp.maximum(running_max, jnp.max(masked, axis=1))
    weights = jnp.where(allowed, jnp.exp(masked - new_max[:, None]), 0.0)
    new_sum = jnp.sum(weights, axis=1)
    new_weighted = jnp.dot(
        weights.astype(jnp.bfloat16), value_part, preferred_element_type=jnp.float32
    )
    return (new_max, new_sum, new_weighted)


def plain_device(hidden, w_query, w_keyvalue, w_output, segment_ids):
    fsdp_count = lax.axis_size("fsdp")
    seq_count = lax.axis_size("sp")
    fsdp_index = lax.axis_index("fsdp")
    seq_index = lax.axis_index("sp")
    tok_rows = hidden.shape[0]
    sub_rows = tok_rows // fsdp_count
    kv_count = seq_count // GROUP
    query_rows = seq_count * sub_rows
    offsets = jnp.arange(query_rows, dtype=jnp.int32)
    query_pos = offsets // sub_rows * tok_rows + fsdp_index * sub_rows + offsets % sub_rows
    own_positions = (
        seq_index * tok_rows + fsdp_index * sub_rows + jnp.arange(sub_rows, dtype=jnp.int32)
    )

    def project(weight_block):
        return jnp.dot(hidden, weight_block, preferred_element_type=jnp.float32)

    query_part = project(lax.all_gather(w_query, "sp", axis=1, tiled=True))
    kv_part = project(lax.all_gather(w_keyvalue, "sp", axis=1, tiled=True))
    query_sum, kv_sum = (
        lax.psum_scatter(query_part, "fsdp", scatter_dimension=0, tiled=True),
        lax.psum_scatter(kv_part, "fsdp", scatter_dimension=0, tiled=True),
    )
    query_local = rotate(query_sum, own_positions, seq_count, HD).astype(jnp.bfloat16)
    pairs = split_keys(kv_sum, own_positions, kv_count, HD)
    expanded = jnp.repeat(pairs, GROUP, axis=1).reshape(sub_rows, seq_count * 2 * HD)
    query_head, kv_head = (
        lax.all_to_all(query_local, "sp", split_axis=1, concat_axis=0, tiled=True),
        lax.all_to_all(expanded, "sp", split_axis=1, concat_axis=0, tiled=True),
    )
    segment_all = lax.all_gather(segment_ids, "sp", axis=0, tiled=True)
    query_seg = segment_all[query_pos]
    initial = (
        jnp.full((query_rows,), NEG_FILL, jnp.float32),
        jnp.zeros((query_rows,), jnp.float32),
        jnp.zeros((query_rows, HD), jnp.float32),
    )
    block_keys = lax.all_gather(kv_head, "fsdp", axis=0, tiled=True)
    piece_rows = block_keys.shape[0]
    row_ids = jnp.arange(piece_rows, dtype=jnp.int32)
    source_id = row_ids // query_rows
    within = row_ids % query_rows
    key_pos = within // sub_rows * tok_rows + source_id * sub_rows + within % sub_rows
    key_seg = segment_all[key_pos]
    final_max, final_sum, final_weighted = merge_keys(
        initial, query_head, query_pos, query_seg, block_keys, key_pos, key_seg
    )
    attention = (final_weighted / final_sum[:, None]).astype(jnp.bfloat16)
    back_rows = lax.all_to_all(attention, "sp", split_axis=0, concat_axis=1, tiled=True)
    mixed_rows = lax.all_gather(back_rows, "fsdp", axis=0, tiled=True)
    result = jnp.dot(
        mixed_rows,
        lax.all_gather(w_output, "sp", axis=0, tiled=True),
        preferred_element_type=jnp.float32,
    )
    return result.astype(jnp.bfloat16)


def turn(lower, upper, cosine, sine_part):
    return lower * cosine - upper * sine_part, upper * cosine + lower * sine_part


def frequencies(index):
    return jnp.exp(index.astype(jnp.float32) * (-2.0 * math.log(ROPE_BASE) / HD))


def row_device(hidden, w_query, w_keyvalue, w_output, segment_ids):
    seq_count = lax.axis_size("sp")
    fsdp_count = lax.axis_size("fsdp")
    x_count = seq_count // fsdp_count
    fsdp_index = lax.axis_index("fsdp")
    seq_index = lax.axis_index("sp")
    z_index = seq_index // x_count
    x_index = seq_index % x_count
    y_index = fsdp_index // 2
    core = fsdp_index % 2
    tok_rows = hidden.shape[0]
    row_tokens = tok_rows * x_count

    def over_sp(value, target):
        pairs = [(i, target(i)) for i in range(seq_count)]
        return lax.ppermute(value, "sp", [(i, t) for i, t in pairs if t < seq_count])

    def z_swap(value, bit):
        return over_sp(value, lambda i: i ^ (bit * x_count))

    def x_swap(value):
        return over_sp(value, lambda i: i ^ 1)

    def core_swap(value):
        return lax.ppermute(value, "fsdp", [(i, i ^ 1) for i in range(fsdp_count)])

    def y_swap(value):
        return lax.ppermute(value, "fsdp", [(i, i ^ 2) for i in range(fsdp_count)])

    def z_gather(block):
        two = z_swap(block, 2)
        one = z_swap(block, 1)
        return [block, one, two, z_swap(two, 1)]

    def pick(values, index):
        return lax.dynamic_index_in_dim(values, index, axis=0, keepdims=False)

    kv_blocks = z_gather(w_keyvalue.T)
    hidden_pair = jnp.concatenate([hidden, x_swap(hidden)], axis=0)
    query_blocks = z_gather(w_query)
    segment_all = lax.all_gather(segment_ids, "sp", axis=0, tiled=True)

    kv_part = lax.dot_general(
        jnp.concatenate(kv_blocks, axis=0),
        hidden_pair,
        (((1,), (1,)), ((), ())),
        preferred_element_type=jnp.float32,
    ).reshape(fsdp_count, -1, row_tokens)
    kv_width = kv_part.shape[1]

    def kind(which):
        return jnp.stack([pick(kv_part, (2 * which) ^ z_index), pick(kv_part, (2 * which + 1) ^ z_index)])

    kv_half = kind(core) + core_swap(kind(1 - core))
    kv_half = kv_half + y_swap(kv_half)
    offsets = jnp.arange(tok_rows, dtype=jnp.int32)

    def positions_of(z_of):
        own = (z_of * x_count + x_index) * tok_rows + offsets
        other = (z_of * x_count + (x_index ^ 1)) * tok_rows + offsets
        return jnp.concatenate([own, other])

    def segments_of(z_of):
        base = jnp.maximum(z_of, 0) * x_count
        own = lax.dynamic_slice_in_dim(segment_all, (base + x_index) * tok_rows, tok_rows)
        other = lax.dynamic_slice_in_dim(segment_all, (base + (x_index ^ 1)) * tok_rows, tok_rows)
        return jnp.concatenate([own, other])

    row_pos = positions_of(z_index)
    row_seg = segments_of(z_index)
    key_frequency = frequencies(x_index * kv_width + jnp.arange(kv_width, dtype=jnp.int32))
    key_angles = key_frequency[:, None] * row_pos.astype(jnp.float32)[None, :]
    is_key = core == 0
    lower, upper = turn(
        kv_half[0],
        kv_half[1],
        jnp.where(is_key, jnp.cos(key_angles), 1.0),
        jnp.where(is_key, jnp.sin(key_angles), 0.0),
    )
    mine = jnp.stack([lower, upper]).astype(jnp.bfloat16)
    from_x = x_swap(mine)
    from_z = over_sp(mine, lambda i: i + x_count)
    from_zx = over_sp(mine, lambda i: (i ^ 1) + x_count)

    def turned_round(value):
        return jnp.concatenate([value[:, :, tok_rows:], value[:, :, :tok_rows]], axis=2)

    own_columns = jnp.concatenate([from_z, mine], axis=2)
    other_columns = jnp.concatenate([turned_round(from_zx), turned_round(from_x)], axis=2)
    first = jnp.where(x_index == 0, own_columns, other_columns)
    second = jnp.where(x_index == 0, other_columns, own_columns)
    kind_all = jnp.stack([first, second], axis=1).reshape(HD, 2 * row_tokens)
    other_kind = core_swap(kind_all)
    keys = jnp.where(is_key, kind_all, other_kind)
    values = jnp.where(is_key, other_kind, kind_all)
    key_pos = jnp.concatenate([positions_of(z_index - 1), row_pos])
    key_seg = jnp.concatenate([segments_of(z_index - 1), row_seg])

    query_part = jnp.stack(
        [jnp.dot(hidden_pair, block, preferred_element_type=jnp.float32) for block in query_blocks]
    ).reshape(2, 2, row_tokens, HD)

    def of_core(which):
        return lax.dynamic_index_in_dim(query_part, which, axis=1, keepdims=False)

    query_sum = of_core(core) + core_swap(of_core(1 - core))
    query_sum = pick(query_sum, y_index) + y_swap(pick(query_sum, 1 - y_index))
    query_angles = row_pos.astype(jnp.float32)[:, None] * frequencies(jnp.arange(HD // 2))[None, :]
    lower, upper = turn(
        query_sum[:, : HD // 2], query_sum[:, HD // 2 :], jnp.cos(query_angles), jnp.sin(query_angles)
    )
    query = jnp.concatenate([lower, upper], axis=1).astype(jnp.bfloat16)

    scores = jnp.dot(query, keys, preferred_element_type=jnp.float32) * HD ** (-0.5)
    allowed = (
        (key_pos[None, :] <= row_pos[:, None])
        & (key_pos[None, :] >= 0)
        & (key_seg[None, :] == row_seg[:, None])
    )
    masked = jnp.where(allowed, scores, NEG_FILL)
    row_max = jnp.max(masked, axis=1, keepdims=True)
    weights = jnp.where(allowed, jnp.exp(masked - row_max), 0.0)
    row_total = jnp.sum(weights, axis=1, keepdims=True)
    weighted = lax.dot_general(
        weights.astype(jnp.bfloat16), values, (((1,), (1,)), ((), ())), preferred_element_type=jnp.float32
    )
    mix = (weighted / row_total).astype(jnp.bfloat16)

    mix_pair = jnp.concatenate([mix[:tok_rows], x_swap(mix[tok_rows:])], axis=1)
    mix_all = lax.all_gather(mix_pair, "fsdp", axis=1, tiled=True)
    output_rows = []
    for block in z_gather(w_output):
        output_rows += [block, x_swap(block)]
    result = jnp.dot(mix_all, jnp.concatenate(output_rows, axis=0), preferred_element_type=jnp.float32)
    return result.astype(jnp.bfloat16)


def solution(mesh):
    seq_count, fsdp_count = mesh.shape["sp"], mesh.shape["fsdp"]
    by_rows = seq_count == GROUP and fsdp_count == 4
    in_specs = (P("sp", "fsdp"), P("fsdp", "sp"), P("fsdp", "sp"), P("sp", "fsdp"), P("sp"))
    out_specs = P("sp", "fsdp")
    return jax.shard_map(
        row_device if by_rows else plain_device,
        mesh=mesh,
        in_specs=in_specs,
        out_specs=out_specs,
        check_vma=False,
    )
```
